8 devices in a mesh: dp: 2 (over z, y), row: 2 (over x), fsdp: 2 (over core).
Axes of the slice: x: 2, y: 2, z: 1, core: 2. Of those that a mesh axis runs over, the one named last changes fastest.
Arguments:
- x_in: bfloat16 [32768, 768], P(('dp', 'row', 'fsdp'))
- dy_out: bfloat16 [32768, 768], P(('dp', 'row', 'fsdp'))
- w_gate: bfloat16 [768, 2048], P(None, ('row', 'fsdp'))
- w_up: bfloat16 [768, 2048], P(None, ('row', 'fsdp'))
- w_down: bfloat16 [2048, 768], P(('row', 'fsdp'))
- g_next: float32 [8, 3, 768, 2048], P(('dp', 'row', 'fsdp'))
Outputs:
- output 1: bfloat16 [32768, 768], P(('dp', 'row', 'fsdp'))
- output 2: float32 [3, 768, 2048], P(None, None, ('row', 'fsdp'))
- output 3: float32 [8, 3, 768, 2048], P(('dp', 'row', 'fsdp'))
All inputs are finite; a program needn't handle non-finite values.
Results may differ from the reference program's by a relative error of at most 0.0108919.
Values are sent between devices in bfloat16 or wider.
A program may use at most 1 GiB of HBM per device.

```python
import jax
import jax.numpy as jnp
from jax import lax
import math

MODEL_DIM = 768
HIDDEN_DIM = 2048
TOKENS_DEV = 4096
DEVICES = 8


def setup_inputs(seed: int = 0) -> dict:
    rand_keys = jax.random.split(jax.random.key(seed), 6)
    act_shape = (DEVICES * TOKENS_DEV, MODEL_DIM)
    in_scale = 1.0 / math.sqrt(MODEL_DIM)
    hid_scale = 1.0 / math.sqrt(HIDDEN_DIM)
    x_in = jax.random.normal(rand_keys[0], act_shape, jnp.float32).astype(jnp.bfloat16)
    dy_out = jax.random.normal(rand_keys[1], act_shape, jnp.float32).astype(jnp.bfloat16)
    w_gate = (jax.random.normal(rand_keys[2], (MODEL_DIM, HIDDEN_DIM), jnp.float32) * in_scale).astype(jnp.bfloat16)
    w_up = (jax.random.normal(rand_keys[3], (MODEL_DIM, HIDDEN_DIM), jnp.float32) * in_scale).astype(jnp.bfloat16)
    w_down = (jax.random.normal(rand_keys[4], (HIDDEN_DIM, MODEL_DIM), jnp.float32) * hid_scale).astype(jnp.bfloat16)
    g_next = jax.random.normal(rand_keys[5], (DEVICES, 3, MODEL_DIM, HIDDEN_DIM), jnp.float32)
    return {"x_in": x_in, "dy_out": dy_out, "w_gate": w_gate, "w_up": w_up, "w_down": w_down, "g_next": g_next}


def local_backward(x_blk, dy_blk, w_gate, w_up, w_down):
    a_pre = jnp.dot(x_blk, w_gate, preferred_element_type=jnp.float32)
    b_pre = jnp.dot(x_blk, w_up, preferred_element_type=jnp.float32)
    sig_a = jax.nn.sigmoid(a_pre)
    silu_a = a_pre * sig_a
    h_act = (silu_a * b_pre).astype(jnp.bfloat16)
    dh_full = jnp.dot(dy_blk, w_down.T, preferred_element_type=jnp.float32)
    da_bf = (dh_full * b_pre * sig_a * (1.0 + a_pre * (1.0 - sig_a))).astype(jnp.bfloat16)
    db_bf = (dh_full * silu_a).astype(jnp.bfloat16)
    dx_acc = jnp.dot(da_bf, w_gate.T, preferred_element_type=jnp.float32) + jnp.dot(db_bf, w_up.T, preferred_element_type=jnp.float32)
    grad_gate = jnp.dot(x_blk.T, da_bf, preferred_element_type=jnp.float32)
    grad_up = jnp.dot(x_blk.T, db_bf, preferred_element_type=jnp.float32)
    grad_down = jnp.dot(dy_blk.T, h_act, preferred_element_type=jnp.float32)
    return dx_acc.astype(jnp.bfloat16), jnp.stack([grad_gate, grad_up, grad_down])


def reference(x_in, dy_out, w_gate, w_up, w_down, g_next):
    x_blocks = x_in.reshape(DEVICES, TOKENS_DEV, MODEL_DIM)
    dy_blocks = dy_out.reshape(DEVICES, TOKENS_DEV, MODEL_DIM)

    def per_device(block_pair):
        return local_backward(block_pair[0], block_pair[1], w_gate, w_up, w_down)

    dx_blocks, dw_local = lax.map(per_device, (x_blocks, dy_blocks))
    dx_in = dx_blocks.reshape(DEVICES * TOKENS_DEV, MODEL_DIM)
    dw_next = jnp.sum(g_next.astype(jnp.bfloat16).astype(jnp.float32), axis=0)
    return (dx_in, dw_next, dw_local)
```

```python
import jax
import jax.numpy as jnp
from jax import lax
from jax.experimental import pallas as pl
from jax.experimental.pallas import tpu as pltpu
from jax.sharding import PartitionSpec as P

MESH = pl.DeviceIdType.MESH
GROUP_AXES = ("row", "fsdp")
ALL_AXES = ("dp", "row", "fsdp")
F32, BF16 = jnp.float32, jnp.bfloat16
CONTRACT_LAST = (((1,), (1,)), ((), ()))
CONTRACT_FIRST = (((0,), (0,)), ((), ()))
TOKENS, MODEL, HIDDEN = 4096, 768, 2048
HALF, SHARD = HIDDEN // 2, HIDDEN // 4
TILE = 512
STEPS = TOKENS // TILE
PIECES = 8
ROWS = 3 * MODEL // PIECES
SUB = ROWS // 2
VMEM_LIMIT = 63 * 2**20


def mm(lhs, rhs, dims=None):
    if dims is None:
        return jnp.dot(lhs, rhs, preferred_element_type=F32)
    return lax.dot_general(lhs, rhs, dims, preferred_element_type=F32)


def tile_backward(x, dy, w1, w3, w2, dw):
    a = mm(x, w1)
    b = mm(x, w3)
    dh = mm(dy, w2, CONTRACT_LAST)
    s = 0.5 * jnp.tanh(0.5 * a) + 0.5
    sa = a * s
    h = (sa * b).astype(BF16)
    da = (dh * b * (s + sa * (1.0 - s))).astype(BF16)
    db = (dh * sa).astype(BF16)
    dx = mm(da, w1, CONTRACT_LAST) + mm(db, w3, CONTRACT_LAST)
    dw[0] += mm(x, da, CONTRACT_FIRST)
    dw[1] += mm(x, db, CONTRACT_FIRST)
    dw[2] += mm(dy, h, CONTRACT_FIRST)
    return dx


def cols(index, width=SHARD):
    return pl.ds(pl.multiple_of(index * width, width), width)


def first_kernel(x_ref, dy_ref, s1, s3, s2, g, dx_ref, dwa_out, o1, o3, o2, q_keep, q_send,
                 w1, w3, w2, dw, gbuf, keep, send_a, recv_a, recv_b,
                 own_sem, wd_send, wd_recv, wx_send, wx_recv, wf_send, wf_recv,
                 g_sem, a_send, a_recv, b_send, b_recv, qk_sem, qs_sem, dw_sem):
    k = pl.program_id(0)
    dp, row, core = lax.axis_index("dp"), lax.axis_index("row"), lax.axis_index("fsdp")
    partner, x_next, y_next = (dp, row, 1 - core), (dp, 1 - row, core), (1 - dp, row, core)
    mine = cols(core)
    theirs = cols(1 - core)

    def remote(src, dst, send, recv, device):
        return pltpu.make_async_remote_copy(src_ref=src, dst_ref=dst, send_sem=send, recv_sem=recv, device_id=device, device_id_type=MESH)

    shards = (s1, s3, s2)
    near = (w1.at[:, mine], w3.at[:, mine], w2.at[mine, :])
    far = (o1.at[:, mine], o3.at[:, mine], o2.at[mine, :])
    own = [pltpu.make_async_copy(shards[i], near[i], own_sem.at[i]) for i in range(3)]
    to_partner = [remote(shards[i], near[i], wd_send.at[i], wd_recv.at[i], partner) for i in range(3)]
    to_x = [remote(shards[i], far[i], wx_send.at[i], wx_recv.at[i], x_next) for i in range(3)]
    forward = [remote(far[i], far[i], wf_send.at[i], wf_recv.at[i], partner) for i in range(3)]

    def load(i):
        return pltpu.make_async_copy(g.at[pl.ds(i * ROWS, ROWS), :], gbuf.at[i % 2], g_sem.at[i % 2])

    def to_a(i):
        return remote(send_a.at[i % 4], recv_a.at[i], a_send.at[i % 4], a_recv.at[i], partner)

    def to_b(i):
        part = keep.at[i, pl.ds(pl.multiple_of((1 - dp) * SUB, SUB), SUB), :]
        return remote(part, recv_b.at[i], b_send.at[i], b_recv.at[i], y_next)

    stay = pl.ds(pl.multiple_of(dp * SUB, SUB), SUB)

    def q_out(i):
        return (pltpu.make_async_copy(keep.at[i, stay, cols(row)], q_keep.at[i], qk_sem.at[i]),
                pltpu.make_async_copy(keep.at[i, stay, cols(1 - row)], q_send.at[i], qs_sem.at[i]))

    def cast(i):
        load(i).wait()
        for half in range(2):
            here = pl.ds(half * SHARD, SHARD)
            keep[i, :, here] = gbuf[i % 2, :, pl.ds(pl.multiple_of(half * HALF + core * SHARD, SHARD), SHARD)].astype(BF16)
            send_a[i % 4, :, here] = gbuf[i % 2, :, pl.ds(pl.multiple_of(half * HALF + (1 - core) * SHARD, SHARD), SHARD)].astype(BF16)
        to_a(i).start()

    def chip_sum(i):
        to_a(i).wait_recv()
        keep[i] = (keep[i].astype(F32) + recv_a[i].astype(F32)).astype(BF16)
        to_b(i).start()

    def pair_sum(i):
        to_b(i).wait_recv()
        keep[i, stay, :] = (keep[i, stay, :].astype(F32) + recv_b[i].astype(F32)).astype(BF16)
        for copy in q_out(i):
            copy.start()

    @pl.when(k == 0)
    def _():
        load(0).start()
        load(1).start()
        for copy in own:
            copy.start()
        barrier = pltpu.get_barrier_semaphore()
        for device in (partner, x_next, y_next):
            pl.semaphore_signal(barrier, inc=1, device_id=device, device_id_type=MESH)
        pl.semaphore_wait(barrier, 3)
        for copy in to_partner + to_x:
            copy.start()
        cast(0)
        load(2).start()
        cast(1)
        load(3).start()
        dw[...] = jnp.zeros_like(dw)
        chip_sum(0)
        for copy in own:
            copy.wait()
        for copy in to_partner:
            copy.wait_recv()

    @pl.when(k <= PIECES - 3)
    def _():
        @pl.when(k >= 2)
        def _():
            to_a(k - 2).wait_send()
        cast(k + 2)

        @pl.when(k <= PIECES - 5)
        def _():
            load(k + 4).start()

    @pl.when(k <= PIECES - 2)
    def _():
        chip_sum(k + 1)

    @pl.when(k >= 2)
    def _():
        pair_sum(k - 2)

    for at, i in ((2, 0), (5, 1), (7, 2)):
        @pl.when(k == at)
        def _():
            to_x[i].wait_recv()
            forward[i].start()

    dx_ref[...] = tile_backward(x_ref[...], dy_ref[...], w1[...], w3[...], w2[...], dw)

    @pl.when(k == STEPS - 1)
    def _():
        dw_copy = pltpu.make_async_copy(dw, dwa_out, dw_sem)
        dw_copy.start()
        pair_sum(PIECES - 2)
        pair_sum(PIECES - 1)
        for i in range(3):
            to_partner[i].wait_send()
            to_x[i].wait_send()
            forward[i].wait_send()
            forward[i].wait_recv()
        for i in range(PIECES - 4, PIECES):
            to_a(i).wait_send()
        for i in range(PIECES):
            to_b(i).wait_send()
            for copy in q_out(i):
                copy.wait()
        dw_copy.wait()


def second_kernel(x_ref, dy_ref, w1, w3, w2, dxp_ref, dwa_ref, dx_ref, dw_out, dw, pass_sem, dw_sem):
    k = pl.program_id(0)
    row = lax.axis_index("row")
    band = MODEL // STEPS
    passing = pltpu.make_async_copy(dwa_ref, dw_out.at[:, pl.ds(pl.multiple_of(k * band, band), band), cols(row, HALF)], pass_sem)
    passing.start()

    @pl.when(k == 0)
    def _():
        dw[...] = jnp.zeros_like(dw)

    dx = tile_backward(x_ref[...], dy_ref[...], w1[...], w3[...], w2[...], dw)
    dx_ref[...] = (dxp_ref[...] + dx).astype(BF16)
    passing.wait()

    @pl.when(k == STEPS - 1)
    def _():
        last = pltpu.make_async_copy(dw, dw_out.at[:, :, cols(1 - row, HALF)], dw_sem)
        last.start()
        last.wait()


def sum_kernel(keep_ref, x_ref, y_ref, d_ref, out_ref):
    dp = lax.axis_index("dp")
    here = pl.ds(pl.multiple_of(dp * SUB, SUB), SUB)
    there = pl.ds(pl.multiple_of((1 - dp) * SUB, SUB), SUB)
    out_ref[0, here, :] = keep_ref[0].astype(F32) + x_ref[0].astype(F32)
    out_ref[0, there, :] = y_ref[0].astype(F32) + d_ref[0].astype(F32)


def solution(mesh):
    any_spec = pl.BlockSpec(memory_space=pl.ANY)
    tile_spec = pl.BlockSpec((TILE, MODEL), lambda t: (t, 0))
    shape = jax.ShapeDtypeStruct
    dma = pltpu.SemaphoreType.DMA
    half_flops = 8 * 2 * TOKENS * MODEL * HALF

    def per_device(x_blk, dy_blk, gate, up, down, g_part):
        g2 = g_part.reshape(3 * MODEL, HIDDEN)
        dxp, dwa, o1, o3, o2, q_keep, q_send = pl.pallas_call(
            first_kernel,
            grid=(STEPS,),
            in_specs=[tile_spec, tile_spec] + [any_spec] * 4,
            out_specs=[tile_spec] + [any_spec] * 6,
            out_shape=[shape((TOKENS, MODEL), F32), shape((3, MODEL, HALF), F32), shape((MODEL, HALF), BF16), shape((MODEL, HALF), BF16),
                       shape((HALF, MODEL), BF16), shape((PIECES, SUB, SHARD), BF16), shape((PIECES, SUB, SHARD), BF16)],
            scratch_shapes=[
                pltpu.VMEM((MODEL, HALF), BF16), pltpu.VMEM((MODEL, HALF), BF16), pltpu.VMEM((HALF, MODEL), BF16),
                pltpu.VMEM((3, MODEL, HALF), F32), pltpu.VMEM((2, ROWS, HIDDEN), F32),
                pltpu.VMEM((PIECES, ROWS, HALF), BF16), pltpu.VMEM((4, ROWS, HALF), BF16), pltpu.VMEM((PIECES, ROWS, HALF), BF16),
                pltpu.VMEM((PIECES, SUB, HALF), BF16),
                dma((3,)), dma((3,)), dma((3,)), dma((3,)), dma((3,)), dma((3,)), dma((3,)),
                dma((2,)), dma((4,)), dma((PIECES,)), dma((PIECES,)), dma((PIECES,)), dma((PIECES,)), dma((PIECES,)), dma,
            ],
            compiler_params=pltpu.CompilerParams(vmem_limit_bytes=VMEM_LIMIT, collective_id=0, has_side_effects=True),
            cost_estimate=pl.CostEstimate(flops=half_flops, bytes_accessed=80 * 2**20, transcendentals=TOKENS * HALF),
            name="near_half",
        )(x_blk, dy_blk, gate, up, down, g2)

        devices = [(d, r, c) for d in range(2) for r in range(2) for c in range(2)]

        def number(d, r, c):
            return 4 * d + 2 * r + c

        from_x = lax.ppermute(q_send, ALL_AXES, [(number(d, r, c), number(d, 1 - r, c)) for d, r, c in devices])
        from_y = lax.ppermute(q_keep, ALL_AXES, [(number(d, r, c), number(1 - d, r, c)) for d, r, c in devices])
        from_diagonal = lax.ppermute(q_send, ALL_AXES, [(number(d, r, c), number(1 - d, 1 - r, c)) for d, r, c in devices])

        whole = pl.BlockSpec(memory_space=pltpu.VMEM)
        dx, dw_local = pl.pallas_call(
            second_kernel,
            grid=(STEPS,),
            in_specs=[tile_spec, tile_spec, whole, whole, whole, tile_spec, pl.BlockSpec((3, MODEL // STEPS, HALF), lambda t: (0, t, 0))],
            out_specs=[tile_spec, any_spec],
            out_shape=[shape((TOKENS, MODEL), BF16), shape((3, MODEL, HIDDEN), F32)],
            scratch_shapes=[pltpu.VMEM((3, MODEL, HALF), F32), dma, dma],
            compiler_params=pltpu.CompilerParams(vmem_limit_bytes=VMEM_LIMIT),
            cost_estimate=pl.CostEstimate(flops=half_flops, bytes_accessed=64 * 2**20, transcendentals=TOKENS * HALF),
            name="far_half",
        )(x_blk, dy_blk, o1, o3, o2, dxp, dwa)

        piece_spec = pl.BlockSpec((1, SUB, SHARD), lambda i: (i, 0, 0))
        dw_next = pl.pallas_call(
            sum_kernel,
            grid=(PIECES,),
            in_specs=[piece_spec] * 4,
            out_specs=pl.BlockSpec((1, ROWS, SHARD), lambda i: (i, 0, 0)),
            out_shape=shape((PIECES, ROWS, SHARD), F32),
            cost_estimate=pl.CostEstimate(flops=2**20, bytes_accessed=10 * 2**20, transcendentals=0),
            name="final_sum",
        )(q_keep, from_x, from_y, from_diagonal)
        return dx, dw_next.reshape(3, MODEL, SHARD), dw_local[None]

    return jax.shard_map(
        per_device,
        mesh=mesh,
        in_specs=(P(ALL_AXES, None), P(ALL_AXES, None), P(None, GROUP_AXES), P(None, GROUP_AXES), P(GROUP_AXES, None), P(ALL_AXES, None, None, None)),
        out_specs=(P(ALL_AXES, None), P(None, None, GROUP_AXES), P(ALL_AXES, None, None, None)),
        check_vma=False,
    )
```

```python
import jax
import jax.numpy as jnp
from jax import lax
from jax.experimental import pallas as pl
from jax.experimental.pallas import tpu as pltpu
from jax.sharding import PartitionSpec as P

MESH = pl.DeviceIdType.MESH
GROUP_AXES = ("row", "fsdp")
ALL_AXES = ("dp", "row", "fsdp")
F32, BF16 = jnp.float32, jnp.bfloat16
CONTRACT_LAST = (((1,), (1,)), ((), ()))
CONTRACT_FIRST = (((0,), (0,)), ((), ()))
TOKENS, MODEL, HIDDEN = 4096, 768, 2048
HALF, SHARD = HIDDEN // 2, HIDDEN // 4
TILE = 512
STEPS = TOKENS // TILE
PIECES = 8
ROWS = 3 * MODEL // PIECES
SUB = ROWS // 2
GROUP = 2
VMEM_LIMIT = 63 * 2**20


def mm(lhs, rhs, dims=None):
    if dims is None:
        return jnp.dot(lhs, rhs, preferred_element_type=F32)
    return lax.dot_general(lhs, rhs, dims, preferred_element_type=F32)


def tile_backward(x, dy, w1, w3, w2, dw, at=slice(None), first=False, flush=None):
    a = mm(x, w1)
    b = mm(x, w3)
    dh = mm(dy, w2, CONTRACT_LAST)
    s = 0.5 * jnp.tanh(0.5 * a) + 0.5
    sa = a * s
    h = (sa * b).astype(BF16)
    da = (dh * b * (s + sa * (1.0 - s))).astype(BF16)
    db = (dh * sa).astype(BF16)
    for i, lhs, rhs in ((2, dy, h), (0, x, da), (1, x, db)):
        grad = mm(lhs, rhs, CONTRACT_FIRST)
        dw[i, :, at] = grad if first else dw[i, :, at] + grad
        if flush is not None:
            flush(i)
    return mm(da, w1, CONTRACT_LAST) + mm(db, w3, CONTRACT_LAST)


def cols(index, width=SHARD):
    return pl.ds(pl.multiple_of(index * width, width), width)


def first_kernel(x_ref, dy_ref, s1, s3, s2, g, dx_ref, dwa_out, o1, o3, o2, q_keep, q_send,
                 w1, w3, w2, dw, gbuf, keep, send_a, recv_a, recv_b,
                 own_sem, wd_send, wd_recv, wx_send, wx_recv, wf_send, wf_recv,
                 g_sem, a_send, a_recv, b_send, b_recv, qk_sem, qs_sem, dw_sem):
    k = pl.program_id(0)
    dp, row, core = lax.axis_index("dp"), lax.axis_index("row"), lax.axis_index("fsdp")
    partner, x_next, y_next = (dp, row, 1 - core), (dp, 1 - row, core), (1 - dp, row, core)
    mine = cols(core)
    theirs = cols(1 - core)

    def remote(src, dst, send, recv, device):
        return pltpu.make_async_remote_copy(src_ref=src, dst_ref=dst, send_sem=send, recv_sem=recv, device_id=device, device_id_type=MESH)

    shards = (s1, s3, s2)
    near = (w1.at[:, mine], w3.at[:, mine], w2.at[mine, :])
    far = (o1.at[:, mine], o3.at[:, mine], o2.at[mine, :])
    own = [pltpu.make_async_copy(shards[i], near[i], own_sem.at[i]) for i in range(3)]
    to_partner = [remote(shards[i], near[i], wd_send.at[i], wd_recv.at[i], partner) for i in range(3)]
    to_x = [remote(shards[i], far[i], wx_send.at[i], wx_recv.at[i], x_next) for i in range(3)]
    forward = [remote(far[i], far[i], wf_send.at[i], wf_recv.at[i], partner) for i in range(3)]

    def load(i):
        return pltpu.make_async_copy(g.at[pl.ds(i * ROWS, ROWS), :], gbuf.at[i % 2], g_sem.at[i % 2])

    def to_a(i):
        return remote(send_a.at[i % 4], recv_a.at[i], a_send.at[i % 4], a_recv.at[i], partner)

    def to_b(i):
        part = keep.at[i, pl.ds(pl.multiple_of((1 - dp) * SUB, SUB), SUB), :]
        return remote(part, recv_b.at[i], b_send.at[i], b_recv.at[i], y_next)

    stay = pl.ds(pl.multiple_of(dp * SUB, SUB), SUB)

    def q_out(i):
        return (pltpu.make_async_copy(keep.at[i, stay, cols(row)], q_keep.at[i], qk_sem.at[i]),
                pltpu.make_async_copy(keep.at[i, stay, cols(1 - row)], q_send.at[i], qs_sem.at[i]))

    def cast(i):
        load(i).wait()
        for half in range(2):
            here = pl.ds(half * SHARD, SHARD)
            keep[i, :, here] = gbuf[i % 2, :, pl.ds(pl.multiple_of(half * HALF + core * SHARD, SHARD), SHARD)].astype(BF16)
            send_a[i % 4, :, here] = gbuf[i % 2, :, pl.ds(pl.multiple_of(half * HALF + (1 - core) * SHARD, SHARD), SHARD)].astype(BF16)
        to_a(i).start()

    def chip_sum(i):
        to_a(i).wait_recv()
        keep[i] = (keep[i].astype(F32) + recv_a[i].astype(F32)).astype(BF16)
        to_b(i).start()

    def pair_sum(i):
        to_b(i).wait_recv()
        keep[i, stay, :] = (keep[i, stay, :].astype(F32) + recv_b[i].astype(F32)).astype(BF16)
        for copy in q_out(i):
            copy.start()

    @pl.when(k == 0)
    def _():
        barrier = pltpu.get_barrier_semaphore()
        for device in (partner, x_next, y_next):
            pl.semaphore_signal(barrier, inc=1, device_id=device, device_id_type=MESH)
        load(0).start()
        for copy in own:
            copy.start()
        load(1).start()
        pl.semaphore_wait(barrier, 3)
        for copy in to_x:
            copy.start()
        cast(0)
        for copy in to_partner:
            copy.start()
        for copy in own:
            copy.wait()
        dx_ref[...] = tile_backward(x_ref[...], dy_ref[...], w1[:, mine], w3[:, mine], w2[mine, :], dw, mine, first=True)
        chip_sum(0)
        cast(1)
        load(2).start()
        for copy in to_partner:
            copy.wait_recv()
        dx_ref[...] += tile_backward(x_ref[...], dy_ref[...], w1[:, theirs], w3[:, theirs], w2[theirs, :], dw, theirs, first=True)

    @pl.when(k > 0)
    def _():
        chip_sum(k)

        @pl.when(k <= PIECES - 2)
        def _():
            @pl.when(k >= 3)
            def _():
                to_a(k - 3).wait_send()
            cast(k + 1)

            @pl.when(k <= PIECES - 3)
            def _():
                load(k + 2).start()

        @pl.when(k >= 2)
        def _():
            pair_sum(k - 2)

        for at, i in ((3, 0), (6, 1)):
            @pl.when(k == at)
            def _():
                to_x[i].wait_recv()
                forward[i].start()

    @pl.when(jnp.logical_and(k > 0, k < STEPS - 1))
    def _():
        dx_ref[...] = tile_backward(x_ref[...], dy_ref[...], w1[...], w3[...], w2[...], dw)

    @pl.when(k == STEPS - 1)
    def _():
        dw_out = [pltpu.make_async_copy(dw.at[i], dwa_out.at[i], dw_sem.at[i]) for i in range(3)]
        dx_ref[...] = tile_backward(x_ref[...], dy_ref[...], w1[...], w3[...], w2[...], dw, flush=lambda i: dw_out[i].start())
        to_x[2].wait_recv()
        forward[2].start()
        pair_sum(PIECES - 2)
        pair_sum(PIECES - 1)
        for i in range(3):
            to_partner[i].wait_send()
            to_x[i].wait_send()
            forward[i].wait_send()
            forward[i].wait_recv()
        for i in range(PIECES - 4, PIECES):
            to_a(i).wait_send()
        for i in range(PIECES):
            to_b(i).wait_send()
            for copy in q_out(i):
                copy.wait()
        for copy in dw_out:
            copy.wait()


def second_kernel(x_ref, dy_ref, w1, w3, w2, dxp_ref, dwa_ref, dx_ref, dw_out, dw, pass_sem, dw_sem):
    k = pl.program_id(0)
    row = lax.axis_index("row")
    band = MODEL // STEPS
    passing = pltpu.make_async_copy(dwa_ref, dw_out.at[:, pl.ds(pl.multiple_of(k * band, band), band), cols(row, HALF)], pass_sem)
    passing.start()

    @pl.when(k == 0)
    def _():
        dw[...] = jnp.zeros_like(dw)

    @pl.when(k < STEPS - 1)
    def _():
        dx = tile_backward(x_ref[...], dy_ref[...], w1[...], w3[...], w2[...], dw)
        dx_ref[...] = (dxp_ref[...] + dx).astype(BF16)

    @pl.when(k == STEPS - 1)
    def _():
        last = [pltpu.make_async_copy(dw.at[i], dw_out.at[i, :, cols(1 - row, HALF)], dw_sem.at[i]) for i in range(3)]
        dx = tile_backward(x_ref[...], dy_ref[...], w1[...], w3[...], w2[...], dw, flush=lambda i: last[i].start())
        dx_ref[...] = (dxp_ref[...] + dx).astype(BF16)
        for copy in last:
            copy.wait()

    passing.wait()


def sum_kernel(keep_ref, x_ref, y_ref, d_ref, out_ref):
    dp = lax.axis_index("dp")
    here = pl.ds(pl.multiple_of(dp * SUB, SUB), SUB)
    there = pl.ds(pl.multiple_of((1 - dp) * SUB, SUB), SUB)
    out_ref[:, here, :] = keep_ref[...].astype(F32) + x_ref[...].astype(F32)
    out_ref[:, there, :] = y_ref[...].astype(F32) + d_ref[...].astype(F32)


def solution(mesh):
    any_spec = pl.BlockSpec(memory_space=pl.ANY)
    tile_spec = pl.BlockSpec((TILE, MODEL), lambda t: (t, 0))
    shape = jax.ShapeDtypeStruct
    dma = pltpu.SemaphoreType.DMA
    half_flops = 8 * 2 * TOKENS * MODEL * HALF

    def per_device(x_blk, dy_blk, gate, up, down, g_part):
        g2 = g_part.reshape(3 * MODEL, HIDDEN)
        dxp, dwa, o1, o3, o2, q_keep, q_send = pl.pallas_call(
            first_kernel,
            grid=(STEPS,),
            in_specs=[tile_spec, tile_spec] + [any_spec] * 4,
            out_specs=[tile_spec] + [any_spec] * 6,
            out_shape=[shape((TOKENS, MODEL), F32), shape((3, MODEL, HALF), F32), shape((MODEL, HALF), BF16), shape((MODEL, HALF), BF16),
                       shape((HALF, MODEL), BF16), shape((PIECES, SUB, SHARD), BF16), shape((PIECES, SUB, SHARD), BF16)],
            scratch_shapes=[
                pltpu.VMEM((MODEL, HALF), BF16), pltpu.VMEM((MODEL, HALF), BF16), pltpu.VMEM((HALF, MODEL), BF16),
                pltpu.VMEM((3, MODEL, HALF), F32), pltpu.VMEM((2, ROWS, HIDDEN), F32),
                pltpu.VMEM((PIECES, ROWS, HALF), BF16), pltpu.VMEM((4, ROWS, HALF), BF16), pltpu.VMEM((PIECES, ROWS, HALF), BF16),
                pltpu.VMEM((PIECES, SUB, HALF), BF16),
                dma((3,)), dma((3,)), dma((3,)), dma((3,)), dma((3,)), dma((3,)), dma((3,)),
                dma((2,)), dma((4,)), dma((PIECES,)), dma((PIECES,)), dma((PIECES,)), dma((PIECES,)), dma((PIECES,)), dma((3,)),
            ],
            compiler_params=pltpu.CompilerParams(vmem_limit_bytes=VMEM_LIMIT, collective_id=0, has_side_effects=True),
            cost_estimate=pl.CostEstimate(flops=half_flops, bytes_accessed=80 * 2**20, transcendentals=TOKENS * HALF),
            name="near_half",
        )(x_blk, dy_blk, gate, up, down, g2)

        devices = [(d, r, c) for d in range(2) for r in range(2) for c in range(2)]

        def number(d, r, c):
            return 4 * d + 2 * r + c

        from_x = lax.ppermute(q_send, ALL_AXES, [(number(d, r, c), number(d, 1 - r, c)) for d, r, c in devices])
        from_y = lax.ppermute(q_keep, ALL_AXES, [(number(d, r, c), number(1 - d, r, c)) for d, r, c in devices])
        from_diagonal = lax.ppermute(q_send, ALL_AXES, [(number(d, r, c), number(1 - d, 1 - r, c)) for d, r, c in devices])

        whole = pl.BlockSpec(memory_space=pltpu.VMEM)
        dx, dw_local = pl.pallas_call(
            second_kernel,
            grid=(STEPS,),
            in_specs=[tile_spec, tile_spec, whole, whole, whole, tile_spec, pl.BlockSpec((3, MODEL // STEPS, HALF), lambda t: (0, t, 0))],
            out_specs=[tile_spec, any_spec],
            out_shape=[shape((TOKENS, MODEL), BF16), shape((3, MODEL, HIDDEN), F32)],
            scratch_shapes=[pltpu.VMEM((3, MODEL, HALF), F32), dma, dma((3,))],
            compiler_params=pltpu.CompilerParams(vmem_limit_bytes=VMEM_LIMIT),
            cost_estimate=pl.CostEstimate(flops=half_flops, bytes_accessed=64 * 2**20, transcendentals=TOKENS * HALF),
            name="far_half",
        )(x_blk, dy_blk, o1, o3, o2, dxp, dwa)

        piece_spec = pl.BlockSpec((GROUP, SUB, SHARD), lambda i: (i, 0, 0))
        dw_next = pl.pallas_call(
            sum_kernel,
            grid=(PIECES // GROUP,),
            in_specs=[piece_spec] * 4,
            out_specs=pl.BlockSpec((GROUP, ROWS, SHARD), lambda i: (i, 0, 0)),
            out_shape=shape((PIECES, ROWS, SHARD), F32),
            cost_estimate=pl.CostEstimate(flops=2**20, bytes_accessed=10 * 2**20, transcendentals=0),
            name="final_sum",
        )(q_keep, from_x, from_y, from_diagonal)
        return dx, dw_next.reshape(3, MODEL, SHARD), dw_local[None]

    return jax.shard_map(
        per_device,
        mesh=mesh,
        in_specs=(P(ALL_AXES, None), P(ALL_AXES, None), P(None, GROUP_AXES), P(None, GROUP_AXES), P(GROUP_AXES, None), P(ALL_AXES, None, None, None)),
        out_specs=(P(ALL_AXES, None), P(None, None, GROUP_AXES), P(ALL_AXES, None, None, None)),
        check_vma=False,
    )
```

```python
import jax
import jax.numpy as jnp
from jax import lax
from jax.experimental import pallas as pl
from jax.experimental.pallas import tpu as pltpu
from jax.sharding import PartitionSpec as P

MESH = pl.DeviceIdType.MESH
GROUP_AXES = ("row", "fsdp")
ALL_AXES = ("dp", "row", "fsdp")
F32, BF16 = jnp.float32, jnp.bfloat16
CONTRACT_LAST = (((1,), (1,)), ((), ()))
CONTRACT_FIRST = (((0,), (0,)), ((), ()))
TOKENS, MODEL, HIDDEN = 4096, 768, 2048
HALF, SHARD = HIDDEN // 2, HIDDEN // 4
TILE = 512
STEPS = TOKENS // TILE
PIECES = 8
ROWS = 3 * MODEL // PIECES
SUB = ROWS // 2
FAR = 4
VMEM_LIMIT = 63 * 2**20


def mm(lhs, rhs, dims=None):
    if dims is None:
        return jnp.dot(lhs, rhs, preferred_element_type=F32)
    return lax.dot_general(lhs, rhs, dims, preferred_element_type=F32)


def tile_backward(x, dy, w1, w3, w2, dw, at=slice(None), first=False, flush=None):
    a = mm(x, w1)
    b = mm(x, w3)
    dh = mm(dy, w2, CONTRACT_LAST)
    s = 0.5 * jnp.tanh(0.5 * a) + 0.5
    sa = a * s
    h = (sa * b).astype(BF16)
    da = (dh * b * (s + sa * (1.0 - s))).astype(BF16)
    db = (dh * sa).astype(BF16)
    for i, lhs, rhs in ((2, dy, h), (0, x, da), (1, x, db)):
        grad = mm(lhs, rhs, CONTRACT_FIRST)
        dw[i, :, at] = grad if first else dw[i, :, at] + grad
        if flush is not None:
            flush(i)
    return mm(da, w1, CONTRACT_LAST) + mm(db, w3, CONTRACT_LAST)


def cols(index, width=SHARD):
    return pl.ds(pl.multiple_of(index * width, width), width)


def first_kernel(x_ref, dy_ref, s1, s3, s2, g, dx_ref, dxp_out, dw_out, o1, o3, o2, fin_own, fin_other,
                 w1, w3, w2, dw, dxs, gbuf, keep, send_a, recv_a, recv_b, recv_c,
                 own_sem, wd_send, wd_recv, wx_send, wx_recv, wf_send, wf_recv, g_sem, a_send, a_recv, b_send, b_recv,
                 c_send, c_recv, f_send, f_recv, fin_sem, dw_sem, dx_sem, o_sem):
    k = pl.program_id(0)
    dp, row, core = lax.axis_index("dp"), lax.axis_index("row"), lax.axis_index("fsdp")
    partner, x_next, y_next = (dp, row, 1 - core), (dp, 1 - row, core), (1 - dp, row, core)
    mine = cols(core)
    theirs = cols(1 - core)
    half = k // STEPS
    slot = k % FAR

    def remote(src, dst, send, recv, device):
        return pltpu.make_async_remote_copy(src_ref=src, dst_ref=dst, send_sem=send, recv_sem=recv, device_id=device, device_id_type=MESH)

    shards = (s1, s3, s2)
    near = (w1.at[0, :, mine], w3.at[0, :, mine], w2.at[0, mine, :])
    far = (w1.at[1, :, mine], w3.at[1, :, mine], w2.at[1, mine, :])
    own = [pltpu.make_async_copy(shards[i], near[i], own_sem.at[i]) for i in range(3)]
    to_partner = [remote(shards[i], near[i], wd_send.at[i], wd_recv.at[i], partner) for i in range(3)]
    to_x = [remote(shards[i], far[i], wx_send.at[i], wx_recv.at[i], x_next) for i in range(3)]
    forward = [remote(far[i], far[i], wf_send.at[i], wf_recv.at[i], partner) for i in range(3)]
    far_out = [pltpu.make_async_copy(w.at[1], o, o_sem.at[i]) for i, (w, o) in enumerate(((w1, o1), (w3, o3), (w2, o2)))]

    def load(i):
        return pltpu.make_async_copy(g.at[pl.ds(i * ROWS, ROWS), :], gbuf.at[i % 2], g_sem.at[i % 2])

    def to_a(i):
        return remote(send_a.at[i % 4], recv_a.at[i], a_send.at[i % 4], a_recv.at[i], partner)

    def to_b(i):
        part = keep.at[i, pl.ds(pl.multiple_of((1 - dp) * SUB, SUB), SUB), :]
        return remote(part, recv_b.at[i], b_send.at[i], b_recv.at[i], y_next)

    stay = pl.ds(pl.multiple_of(dp * SUB, SUB), SUB)

    def to_c(i):
        return remote(keep.at[i, stay, cols(1 - row)], recv_c.at[i], c_send.at[i], c_recv.at[i], x_next)

    def to_f(i):
        return remote(keep.at[i, stay, cols(row)], fin_other.at[i], f_send.at[i], f_recv.at[i], y_next)

    def own_fin(i):
        return pltpu.make_async_copy(keep.at[i, stay, cols(row)], fin_own.at[i], fin_sem.at[i])

    def dx_out(i):
        return pltpu.make_async_copy(dxs.at[i], dxp_out.at[i], dx_sem.at[i])

    def cast(i):
        load(i).wait()
        for part in range(2):
            here = pl.ds(part * SHARD, SHARD)
            keep[i, :, here] = gbuf[i % 2, :, pl.ds(pl.multiple_of(part * HALF + core * SHARD, SHARD), SHARD)].astype(BF16)
            send_a[i % 4, :, here] = gbuf[i % 2, :, pl.ds(pl.multiple_of(part * HALF + (1 - core) * SHARD, SHARD), SHARD)].astype(BF16)
        to_a(i).start()

    def chip_sum(i):
        to_a(i).wait_recv()
        keep[i] = (keep[i].astype(F32) + recv_a[i].astype(F32)).astype(BF16)
        to_b(i).start()

    def pair_sum(i):
        to_b(i).wait_recv()
        keep[i, stay, :] = (keep[i, stay, :].astype(F32) + recv_b[i].astype(F32)).astype(BF16)
        to_c(i).start()

    def whole_sum(i):
        to_c(i).wait_recv()
        keep[i, stay, cols(row)] = (keep[i, stay, cols(row)].astype(F32) + recv_c[i].astype(F32)).astype(BF16)
        to_f(i).start()
        own_fin(i).start()

    @pl.when(k == 0)
    def _():
        barrier = pltpu.get_barrier_semaphore()
        for device in (partner, x_next, y_next):
            pl.semaphore_signal(barrier, inc=1, device_id=device, device_id_type=MESH)
        load(0).start()
        for copy in own:
            copy.start()
        load(1).start()
        pl.semaphore_wait(barrier, 3)
        for copy in to_x:
            copy.start()
        cast(0)
        for copy in to_partner:
            copy.start()
        for copy in own:
            copy.wait()
        dxs[0] = tile_backward(x_ref[...], dy_ref[...], w1[0, :, mine], w3[0, :, mine], w2[0, mine, :], dw, mine, first=True)
        chip_sum(0)
        cast(1)
        load(2).start()
        for copy in to_partner:
            copy.wait_recv()
        dxs[0] += tile_backward(x_ref[...], dy_ref[...], w1[0, :, theirs], w3[0, :, theirs], w2[0, theirs, :], dw, theirs, first=True)

    @pl.when(jnp.logical_and(k > 0, k < PIECES))
    def _():
        chip_sum(k)

        @pl.when(k <= PIECES - 2)
        def _():
            @pl.when(k >= 3)
            def _():
                to_a(k - 3).wait_send()
            cast(k + 1)

            @pl.when(k <= PIECES - 3)
            def _():
                load(k + 2).start()

        @pl.when(k <= FAR)
        def _():
            dx_out(k - 1).start()

        @pl.when(k >= FAR)
        def _():
            dx_out(k - FAR).wait()

        for at, i in ((3, 0), (5, 1), (7, 2)):
            @pl.when(k == at)
            def _():
                to_x[i].wait_recv()
                forward[i].start()

    @pl.when(jnp.logical_and(k >= 2, k <= PIECES + 1))
    def _():
        pair_sum(k - 2)

    @pl.when(k >= STEPS)
    def _():
        @pl.when(k == STEPS)
        def _():
            for i in range(3):
                forward[i].wait_recv()
                far_out[i].start()
            for i in range(3):
                pltpu.make_async_copy(dw.at[i], dw_out.at[0, i], dw_sem.at[i]).wait()
            dw[...] = jnp.zeros_like(dw)
        whole_sum(2 * (k - STEPS))
        whole_sum(2 * (k - STEPS) + 1)

    def finish(flush):
        dx = tile_backward(x_ref[...], dy_ref[...], w1[half], w3[half], w2[half], dw, flush=flush)
        total = dx + jnp.where(k >= STEPS, dxs[slot], 0.0)
        dxs[slot] = total
        dx_ref[...] = total.astype(BF16)

    ends = jnp.logical_or(k == STEPS - 1, k == STEPS + FAR - 1)

    @pl.when(jnp.logical_and(k > 0, jnp.logical_not(ends)))
    def _():
        finish(None)

    @pl.when(ends)
    def _():
        finish(lambda i: pltpu.make_async_copy(dw.at[i], dw_out.at[half, i], dw_sem.at[i]).start())

    @pl.when(k == STEPS + FAR - 1)
    def _():
        for i in range(3):
            to_partner[i].wait_send()
            to_x[i].wait_send()
            forward[i].wait_send()
            far_out[i].wait()
        for i in range(PIECES - 4, PIECES):
            to_a(i).wait_send()
        for i in range(PIECES):
            to_b(i).wait_send()
            to_c(i).wait_send()
            own_fin(i).wait()
            to_f(i).wait()
        for i in range(3):
            pltpu.make_async_copy(dw.at[i], dw_out.at[1, i], dw_sem.at[i]).wait()


def second_kernel(x_ref, dy_ref, w1, w3, w2, dxp_ref, dxq_ref, own_ref, other_ref, dw_part, dx_ref, next_ref, dw_out,
                  dw, near_buf, far_buf, near_in_sem, near_out_sem, far_in_sem, far_out_sem):
    k = pl.program_id(0)
    dp, row = lax.axis_index("dp"), lax.axis_index("row")
    near_in = [pltpu.make_async_copy(dw_part.at[0, i], near_buf.at[i], near_in_sem.at[i]) for i in range(3)]
    near_out = [pltpu.make_async_copy(near_buf.at[i], dw_out.at[i, :, cols(row, HALF)], near_out_sem.at[i]) for i in range(3)]
    far_in = [pltpu.make_async_copy(dw_part.at[1, i], far_buf.at[i], far_in_sem.at[i]) for i in range(3)]
    far_out = [pltpu.make_async_copy(dw.at[i], dw_out.at[i, :, cols(1 - row, HALF)], far_out_sem.at[i]) for i in range(3)]

    @pl.when(k == 0)
    def _():
        for copy in far_in + near_in:
            copy.start()
        dw[...] = jnp.zeros_like(dw)

    for i in range(3):
        @pl.when(k == i + 1)
        def _():
            far_in[i].wait()
            dw[i] += far_buf[i]
            near_in[i].wait()
            near_out[i].start()

    next_ref[:, pl.ds(pl.multiple_of(dp * SUB, SUB), SUB), :] = own_ref[...].astype(F32)
    next_ref[:, pl.ds(pl.multiple_of((1 - dp) * SUB, SUB), SUB), :] = other_ref[...].astype(F32)
    dx_ref[1] = dxq_ref[...]

    def finish(flush):
        dx = tile_backward(x_ref[...], dy_ref[...], w1[...], w3[...], w2[...], dw, flush=flush)
        dx_ref[0] = (dxp_ref[0] + dx).astype(BF16)

    @pl.when(k < FAR - 1)
    def _():
        finish(None)

    @pl.when(k == FAR - 1)
    def _():
        finish(lambda i: far_out[i].start())
        for copy in near_out + far_out:
            copy.wait()


def solution(mesh):
    any_spec = pl.BlockSpec(memory_space=pl.ANY)
    whole = pl.BlockSpec(memory_space=pltpu.VMEM)
    shape = jax.ShapeDtypeStruct
    dma = pltpu.SemaphoreType.DMA
    rest = STEPS - FAR
    tile_flops = 8 * 2 * TILE * MODEL * HALF

    def per_device(x_blk, dy_blk, gate, up, down, g_part):
        g2 = g_part.reshape(3 * MODEL, HIDDEN)
        spec = pl.BlockSpec((TILE, MODEL), lambda t: (jnp.where(t < STEPS, t, t - FAR), 0))
        dxq, dxp, dw_part, o1, o3, o2, fin_own, fin_other = pl.pallas_call(
            first_kernel,
            grid=(STEPS + FAR,),
            in_specs=[spec, spec] + [any_spec] * 4,
            out_specs=[pl.BlockSpec((TILE, MODEL), lambda t: (jnp.maximum(t - STEPS, 0), 0))] + [any_spec] * 7,
            out_shape=[shape((FAR * TILE, MODEL), BF16), shape((rest, TILE, MODEL), F32), shape((2, 3, MODEL, HALF), F32),
                       shape((MODEL, HALF), BF16), shape((MODEL, HALF), BF16), shape((HALF, MODEL), BF16),
                       shape((PIECES, SUB, SHARD), BF16), shape((PIECES, SUB, SHARD), BF16)],
            scratch_shapes=[
                pltpu.VMEM((2, MODEL, HALF), BF16), pltpu.VMEM((2, MODEL, HALF), BF16), pltpu.VMEM((2, HALF, MODEL), BF16),
                pltpu.VMEM((3, MODEL, HALF), F32), pltpu.VMEM((FAR, TILE, MODEL), F32), pltpu.VMEM((2, ROWS, HIDDEN), F32),
                pltpu.VMEM((PIECES, ROWS, HALF), BF16), pltpu.VMEM((4, ROWS, HALF), BF16), pltpu.VMEM((PIECES, ROWS, HALF), BF16),
                pltpu.VMEM((PIECES, SUB, HALF), BF16), pltpu.VMEM((PIECES, SUB, SHARD), BF16),
            ] + [dma((3,))] * 7 + [dma((2,)), dma((4,))] + [dma((PIECES,))] * 8 + [dma((3,)), dma((rest,)), dma((3,))],
            compiler_params=pltpu.CompilerParams(vmem_limit_bytes=VMEM_LIMIT, collective_id=0, has_side_effects=True),
            cost_estimate=pl.CostEstimate(flops=(STEPS + FAR) * tile_flops, bytes_accessed=100 * 2**20, transcendentals=TOKENS * HALF),
            name="near_and_far",
        )(x_blk, dy_blk, gate, up, down, g2)

        tile_spec = pl.BlockSpec((TILE, MODEL), lambda t: (t, 0))
        piece_spec = pl.BlockSpec((PIECES // rest, SUB, SHARD), lambda t: (t, 0, 0))
        dx, dw_next, dw_local = pl.pallas_call(
            second_kernel,
            grid=(rest,),
            in_specs=[tile_spec, tile_spec, whole, whole, whole, pl.BlockSpec((1, TILE, MODEL), lambda t: (t, 0, 0)), tile_spec, piece_spec, piece_spec, any_spec],
            out_specs=[pl.BlockSpec((2, TILE, MODEL), lambda t: (0, t, 0)), pl.BlockSpec((PIECES // rest, ROWS, SHARD), lambda t: (t, 0, 0)), any_spec],
            out_shape=[shape((2, TOKENS // 2, MODEL), BF16), shape((PIECES, ROWS, SHARD), F32), shape((3, MODEL, HIDDEN), F32)],
            scratch_shapes=[pltpu.VMEM((3, MODEL, HALF), F32)] * 3 + [dma((3,))] * 4,
            compiler_params=pltpu.CompilerParams(vmem_limit_bytes=VMEM_LIMIT),
            cost_estimate=pl.CostEstimate(flops=rest * tile_flops, bytes_accessed=70 * 2**20, transcendentals=TOKENS * HALF // 2),
            name="far_rest",
        )(x_blk, dy_blk, o1, o3, o2, dxp, dxq, fin_own, fin_other, dw_part)
        return dx.reshape(TOKENS, MODEL), dw_next.reshape(3, MODEL, SHARD), dw_local[None]

    return jax.shard_map(
        per_device,
        mesh=mesh,
        in_specs=(P(ALL_AXES, None), P(ALL_AXES, None), P(None, GROUP_AXES), P(None, GROUP_AXES), P(GROUP_AXES, None), P(ALL_AXES, None, None, None)),
        out_specs=(P(ALL_AXES, None), P(None, None, GROUP_AXES), P(ALL_AXES, None, None, None)),
        check_vma=False,
    )
```

```python
import jax
import jax.numpy as jnp
from jax import lax
from jax.experimental import pallas as pl
from jax.experimental.pallas import tpu as pltpu
from jax.sharding import PartitionSpec as P

MESH = pl.DeviceIdType.MESH
GROUP_AXES = ("row", "fsdp")
ALL_AXES = ("dp", "row", "fsdp")
F32, BF16 = jnp.float32, jnp.bfloat16
CONTRACT_LAST = (((1,), (1,)), ((), ()))
CONTRACT_FIRST = (((0,), (0,)), ((), ()))
TOKENS, MODEL, HIDDEN = 4096, 768, 2048
HALF, SHARD = HIDDEN // 2, HIDDEN // 4
TILE = 512
STEPS = TOKENS // TILE
PIECES = 8
ROWS = 3 * MODEL // PIECES
SUB = ROWS // 2
FAR = 4
VMEM_LIMIT = 63 * 2**20


def mm(lhs, rhs, dims=None):
    if dims is None:
        return jnp.dot(lhs, rhs, preferred_element_type=F32)
    return lax.dot_general(lhs, rhs, dims, preferred_element_type=F32)


def tile_backward(x, dy, w1, w3, w2, dw, at=slice(None), first=False, flush=None):
    a = mm(x, w1)
    b = mm(x, w3)
    dh = mm(dy, w2, CONTRACT_LAST)
    s = 0.5 * jnp.tanh(0.5 * a) + 0.5
    sa = a * s
    h = (sa * b).astype(BF16)
    da = (dh * b * (s + sa * (1.0 - s))).astype(BF16)
    db = (dh * sa).astype(BF16)
    for i, lhs, rhs in ((2, dy, h), (0, x, da), (1, x, db)):
        grad = mm(lhs, rhs, CONTRACT_FIRST)
        dw[i, :, at] = grad if first else dw[i, :, at] + grad
        if flush is not None:
            flush(i)
    return mm(da, w1, CONTRACT_LAST) + mm(db, w3, CONTRACT_LAST)


def cols(index, width=SHARD):
    return pl.ds(pl.multiple_of(index * width, width), width)


def first_kernel(x_hbm, dy_hbm, s1, s3, s2, g, dx_ref, dxp_out, dw_out, o1, o3, o2, fin_own, fin_other,
                 w1, w3, w2, dw, dxs, gbuf, keep, send_a, recv_a, recv_b, recv_c, xs, dys,
                 own_sem, wd_send, wd_recv, wx_send, wx_recv, wf_send, wf_recv, g_sem, a_send, a_recv, b_send, b_recv,
                 c_send, c_recv, f_send, f_recv, fin_sem, dw_sem, dx_sem, o_sem, x_sem, dy_sem):
    k = pl.program_id(0)
    dp, row, core = lax.axis_index("dp"), lax.axis_index("row"), lax.axis_index("fsdp")
    partner, x_next, y_next = (dp, row, 1 - core), (dp, 1 - row, core), (1 - dp, row, core)
    mine = cols(core)
    theirs = cols(1 - core)
    half = k // STEPS
    slot = k % FAR

    def remote(src, dst, send, recv, device):
        return pltpu.make_async_remote_copy(src_ref=src, dst_ref=dst, send_sem=send, recv_sem=recv, device_id=device, device_id_type=MESH)

    shards = (s1, s3, s2)
    near = (w1.at[0, :, mine], w3.at[0, :, mine], w2.at[0, mine, :])
    far = (w1.at[1, :, mine], w3.at[1, :, mine], w2.at[1, mine, :])
    own = [pltpu.make_async_copy(shards[i], near[i], own_sem.at[i]) for i in range(3)]
    to_partner = [remote(shards[i], near[i], wd_send.at[i], wd_recv.at[i], partner) for i in range(3)]
    to_x = [remote(shards[i], far[i], wx_send.at[i], wx_recv.at[i], x_next) for i in range(3)]
    forward = [remote(far[i], far[i], wf_send.at[i], wf_recv.at[i], partner) for i in range(3)]
    far_out = [pltpu.make_async_copy(w.at[1], o, o_sem.at[i]) for i, (w, o) in enumerate(((w1, o1), (w3, o3), (w2, o2)))]

    def tokens(i):
        rows = pl.ds(pl.multiple_of(jnp.where(i < STEPS, i, i - FAR) * TILE, TILE), TILE)
        return (pltpu.make_async_copy(x_hbm.at[rows, :], xs.at[i % 2], x_sem.at[i % 2]),
                pltpu.make_async_copy(dy_hbm.at[rows, :], dys.at[i % 2], dy_sem.at[i % 2]))

    def load(i):
        return pltpu.make_async_copy(g.at[pl.ds(i * ROWS, ROWS), :], gbuf.at[i % 2], g_sem.at[i % 2])

    def to_a(i):
        return remote(send_a.at[i % 4], recv_a.at[i], a_send.at[i % 4], a_recv.at[i], partner)

    def to_b(i):
        part = keep.at[i, pl.ds(pl.multiple_of((1 - dp) * SUB, SUB), SUB), :]
        return remote(part, recv_b.at[i], b_send.at[i], b_recv.at[i], y_next)

    stay = pl.ds(pl.multiple_of(dp * SUB, SUB), SUB)

    def to_c(i):
        return remote(keep.at[i, stay, cols(1 - row)], recv_c.at[i], c_send.at[i], c_recv.at[i], x_next)

    def to_f(i):
        return remote(keep.at[i, stay, cols(row)], fin_other.at[i], f_send.at[i], f_recv.at[i], y_next)

    def own_fin(i):
        return pltpu.make_async_copy(keep.at[i, stay, cols(row)], fin_own.at[i], fin_sem.at[i])

    def dx_out(i):
        return pltpu.make_async_copy(dxs.at[i], dxp_out.at[i], dx_sem.at[i])

    def cast(i):
        load(i).wait()
        for part in range(2):
            here = pl.ds(part * SHARD, SHARD)
            keep[i, :, here] = gbuf[i % 2, :, pl.ds(pl.multiple_of(part * HALF + core * SHARD, SHARD), SHARD)].astype(BF16)
            send_a[i % 4, :, here] = gbuf[i % 2, :, pl.ds(pl.multiple_of(part * HALF + (1 - core) * SHARD, SHARD), SHARD)].astype(BF16)
        to_a(i).start()

    def chip_sum(i):
        to_a(i).wait_recv()
        keep[i] = keep[i] + recv_a[i]
        to_b(i).start()

    def pair_sum(i):
        to_b(i).wait_recv()
        keep[i, stay, :] = keep[i, stay, :] + recv_b[i]
        to_c(i).start()

    def whole_sum(i):
        to_c(i).wait_recv()
        keep[i, stay, cols(row)] = keep[i, stay, cols(row)] + recv_c[i]
        to_f(i).start()
        own_fin(i).start()

    @pl.when(k == 0)
    def _():
        barrier = pltpu.get_barrier_semaphore()
        for device in (partner, x_next, y_next):
            pl.semaphore_signal(barrier, inc=1, device_id=device, device_id_type=MESH)
        for copy in tokens(0):
            copy.start()
        for copy in own:
            copy.start()
        pl.semaphore_wait(barrier, 3)
        for copy in to_x:
            copy.start()
        for copy in tokens(0):
            copy.wait()
        for copy in own:
            copy.wait()
        for copy in to_partner:
            copy.start()
        load(0).start()
        load(1).start()
        for copy in tokens(1):
            copy.start()
        dxs[0] = tile_backward(xs[0], dys[0], w1[0, :, mine], w3[0, :, mine], w2[0, mine, :], dw, mine, first=True)
        cast(0)
        load(2).start()
        cast(1)
        load(3).start()
        for copy in to_partner:
            copy.wait_recv()
        dxs[0] += tile_backward(xs[0], dys[0], w1[0, :, theirs], w3[0, :, theirs], w2[0, theirs, :], dw, theirs, first=True)

    @pl.when(k > 0)
    def _():
        for copy in tokens(k):
            copy.wait()

        @pl.when(k < STEPS + FAR - 1)
        def _():
            for copy in tokens(k + 1):
                copy.start()

    @pl.when(k == 1)
    def _():
        chip_sum(0)

    @pl.when(jnp.logical_and(k > 0, k < PIECES))
    def _():
        chip_sum(k)

        @pl.when(k <= PIECES - 2)
        def _():
            @pl.when(k >= 3)
            def _():
                to_a(k - 3).wait_send()
            cast(k + 1)

            @pl.when(k <= PIECES - 4)
            def _():
                load(k + 3).start()

        @pl.when(k <= FAR)
        def _():
            dx_out(k - 1).start()

        @pl.when(k >= FAR)
        def _():
            dx_out(k - FAR).wait()

        for at, i in ((3, 0), (6, 1)):
            @pl.when(k == at)
            def _():
                to_x[i].wait_recv()
                forward[i].start()

    @pl.when(jnp.logical_and(k >= 3, k <= PIECES + 1))
    def _():
        @pl.when(k == 3)
        def _():
            pair_sum(0)
        pair_sum(k - 2)

    @pl.when(k >= STEPS)
    def _():
        for at, pieces in enumerate(((0, 1), (2, 3), (4, 5, 6), (7,))):
            @pl.when(k == STEPS + at)
            def _():
                for i in pieces:
                    whole_sum(i)

        @pl.when(k == STEPS)
        def _():
            for i in range(3):
                pltpu.make_async_copy(dw.at[i], dw_out.at[0, i], dw_sem.at[i]).wait()
            dw[...] = jnp.zeros_like(dw)
            for i in range(3):
                forward[i].wait_recv()
                far_out[i].start()

    def finish(flush):
        dx = tile_backward(xs[k % 2], dys[k % 2], w1[half], w3[half], w2[half], dw, flush=flush)
        total = dx + jnp.where(k >= STEPS, dxs[slot], 0.0)
        dxs[slot] = total
        dx_ref[...] = total.astype(BF16)

    ends = jnp.logical_or(k == STEPS - 1, k == STEPS + FAR - 1)

    @pl.when(jnp.logical_and(k > 0, jnp.logical_not(ends)))
    def _():
        finish(None)

    @pl.when(ends)
    def _():
        finish(lambda i: pltpu.make_async_copy(dw.at[i], dw_out.at[half, i], dw_sem.at[i]).start())

    @pl.when(k == STEPS - 1)
    def _():
        to_x[2].wait_recv()
        forward[2].start()

    @pl.when(k == STEPS + FAR - 1)
    def _():
        for i in range(3):
            to_partner[i].wait_send()
            to_x[i].wait_send()
            forward[i].wait_send()
            far_out[i].wait()
        for i in range(PIECES - 4, PIECES):
            to_a(i).wait_send()
        for i in range(PIECES):
            to_b(i).wait_send()
            to_c(i).wait_send()
            own_fin(i).wait()
            to_f(i).wait()
        for i in range(3):
            pltpu.make_async_copy(dw.at[i], dw_out.at[1, i], dw_sem.at[i]).wait()


def second_kernel(x_hbm, dy_hbm, o1, o3, o2, dxp, dxq, fin_own, fin_other, dw_part, dx_ref, next_ref, dw_out,
                  w1, w3, w2, dw, near_buf, far_buf, xs, dys, dx_near, dx_done, own, other,
                  in_sem, w_sem, near_in_sem, near_out_sem, far_in_sem, far_out_sem):
    k = pl.program_id(0)
    dp, row = lax.axis_index("dp"), lax.axis_index("row")
    slot = k % 2
    near_in = [pltpu.make_async_copy(dw_part.at[0, i], near_buf.at[i], near_in_sem.at[i]) for i in range(3)]
    near_out = [pltpu.make_async_copy(near_buf.at[i], dw_out.at[i, :, cols(row, HALF)], near_out_sem.at[i]) for i in range(3)]
    far_in = [pltpu.make_async_copy(dw_part.at[1, i], far_buf.at[i], far_in_sem.at[i]) for i in range(3)]
    far_out = [pltpu.make_async_copy(dw.at[i], dw_out.at[i, :, cols(1 - row, HALF)], far_out_sem.at[i]) for i in range(3)]
    weights = [pltpu.make_async_copy(o, w, w_sem.at[i]) for i, (o, w) in enumerate(((o1, w1), (o3, w3), (o2, w2)))]
    group = PIECES // (STEPS - FAR)

    def inputs(t):
        rows = pl.ds(pl.multiple_of(t * TILE, TILE), TILE)
        pieces = pl.ds(t * group, group)
        pairs = ((x_hbm.at[rows, :], xs), (dy_hbm.at[rows, :], dys), (dxp.at[t], dx_near), (dxq.at[rows, :], dx_done),
                 (fin_own.at[pieces], own), (fin_other.at[pieces], other))
        return [pltpu.make_async_copy(src, dst.at[t % 2], in_sem.at[t % 2, i]) for i, (src, dst) in enumerate(pairs)]

    @pl.when(k == 0)
    def _():
        now = inputs(0)
        for copy in now[:2] + weights + now[2:]:
            copy.start()
        dw[...] = jnp.zeros_like(dw)
        for copy in weights:
            copy.wait()

    @pl.when(jnp.logical_and(k > 0, k < STEPS - FAR - 1))
    def _():
        for copy in inputs(k + 1):
            copy.start()

    for copy in inputs(k):
        copy.wait()

    @pl.when(k == 0)
    def _():
        for copy in inputs(1) + far_in + near_in:
            copy.start()

    for i in range(3):
        @pl.when(k == i + 1)
        def _():
            far_in[i].wait()
            dw[i] += far_buf[i]
            near_in[i].wait()
            near_out[i].start()

    def finish(flush):
        dx = tile_backward(xs[slot], dys[slot], w1[...], w3[...], w2[...], dw, flush=flush)
        dx_ref[0] = (dx_near[slot] + dx).astype(BF16)
        dx_ref[1] = dx_done[slot]
        next_ref[:, pl.ds(pl.multiple_of(dp * SUB, SUB), SUB), :] = own[slot].astype(F32)
        next_ref[:, pl.ds(pl.multiple_of((1 - dp) * SUB, SUB), SUB), :] = other[slot].astype(F32)

    @pl.when(k < STEPS - FAR - 1)
    def _():
        finish(None)

    @pl.when(k == STEPS - FAR - 1)
    def _():
        finish(lambda i: far_out[i].start())
        for copy in near_out + far_out:
            copy.wait()


def solution(mesh):
    any_spec = pl.BlockSpec(memory_space=pl.ANY)
    shape = jax.ShapeDtypeStruct
    dma = pltpu.SemaphoreType.DMA
    rest = STEPS - FAR
    tile_flops = 8 * 2 * TILE * MODEL * HALF

    def per_device(x_blk, dy_blk, gate, up, down, g_part):
        g2 = g_part.reshape(3 * MODEL, HIDDEN)
        dxq, dxp, dw_part, o1, o3, o2, fin_own, fin_other = pl.pallas_call(
            first_kernel,
            grid=(STEPS + FAR,),
            in_specs=[any_spec] * 6,
            out_specs=[pl.BlockSpec((TILE, MODEL), lambda t: (jnp.maximum(t - STEPS, 0), 0))] + [any_spec] * 7,
            out_shape=[shape((FAR * TILE, MODEL), BF16), shape((rest, TILE, MODEL), F32), shape((2, 3, MODEL, HALF), F32),
                       shape((MODEL, HALF), BF16), shape((MODEL, HALF), BF16), shape((HALF, MODEL), BF16),
                       shape((PIECES, SUB, SHARD), BF16), shape((PIECES, SUB, SHARD), BF16)],
            scratch_shapes=[
                pltpu.VMEM((2, MODEL, HALF), BF16), pltpu.VMEM((2, MODEL, HALF), BF16), pltpu.VMEM((2, HALF, MODEL), BF16),
                pltpu.VMEM((3, MODEL, HALF), F32), pltpu.VMEM((FAR, TILE, MODEL), F32), pltpu.VMEM((2, ROWS, HIDDEN), F32),
                pltpu.VMEM((PIECES, ROWS, HALF), BF16), pltpu.VMEM((4, ROWS, HALF), BF16), pltpu.VMEM((PIECES, ROWS, HALF), BF16),
                pltpu.VMEM((PIECES, SUB, HALF), BF16), pltpu.VMEM((PIECES, SUB, SHARD), BF16),
                pltpu.VMEM((2, TILE, MODEL), BF16), pltpu.VMEM((2, TILE, MODEL), BF16),
            ] + [dma((3,))] * 7 + [dma((2,)), dma((4,))] + [dma((PIECES,))] * 8 + [dma((3,)), dma((rest,)), dma((3,)), dma((2,)), dma((2,))],
            compiler_params=pltpu.CompilerParams(vmem_limit_bytes=VMEM_LIMIT, collective_id=0, has_side_effects=True),
            cost_estimate=pl.CostEstimate(flops=(STEPS + FAR) * tile_flops, bytes_accessed=100 * 2**20, transcendentals=TOKENS * HALF),
            name="near_and_far",
        )(x_blk, dy_blk, gate, up, down, g2)

        dx, dw_next, dw_local = pl.pallas_call(
            second_kernel,
            grid=(rest,),
            in_specs=[any_spec] * 10,
            out_specs=[pl.BlockSpec((2, TILE, MODEL), lambda t: (0, t, 0)), pl.BlockSpec((PIECES // rest, ROWS, SHARD), lambda t: (t, 0, 0)), any_spec],
            out_shape=[shape((2, TOKENS // 2, MODEL), BF16), shape((PIECES, ROWS, SHARD), F32), shape((3, MODEL, HIDDEN), F32)],
            scratch_shapes=[pltpu.VMEM((MODEL, HALF), BF16), pltpu.VMEM((MODEL, HALF), BF16), pltpu.VMEM((HALF, MODEL), BF16)]
            + [pltpu.VMEM((3, MODEL, HALF), F32)] * 3
            + [pltpu.VMEM((2, TILE, MODEL), BF16), pltpu.VMEM((2, TILE, MODEL), BF16), pltpu.VMEM((2, TILE, MODEL), F32), pltpu.VMEM((2, TILE, MODEL), BF16)]
            + [pltpu.VMEM((2, PIECES // rest, SUB, SHARD), BF16)] * 2 + [dma((2, 6))] + [dma((3,))] * 5,
            compiler_params=pltpu.CompilerParams(vmem_limit_bytes=VMEM_LIMIT),
            cost_estimate=pl.CostEstimate(flops=rest * tile_flops, bytes_accessed=70 * 2**20, transcendentals=TOKENS * HALF // 2),
            name="far_rest",
        )(x_blk, dy_blk, o1, o3, o2, dxp, dxq, fin_own, fin_other, dw_part)
        return dx.reshape(TOKENS, MODEL), dw_next.reshape(3, MODEL, SHARD), dw_local[None]

    return jax.shard_map(
        per_device,
        mesh=mesh,
        in_specs=(P(ALL_AXES, None), P(ALL_AXES, None), P(None, GROUP_AXES), P(None, GROUP_AXES), P(GROUP_AXES, None), P(ALL_AXES, None, None, None)),
        out_specs=(P(ALL_AXES, None), P(None, None, GROUP_AXES), P(ALL_AXES, None, None, None)),
        check_vma=False,
    )
```

```python
import jax
import jax.numpy as jnp
from jax import lax
from jax.experimental import pallas as pl
from jax.experimental.pallas import tpu as pltpu
from jax.sharding import PartitionSpec as P

MESH = pl.DeviceIdType.MESH
GROUP_AXES = ("row", "fsdp")
ALL_AXES = ("dp", "row", "fsdp")
F32, BF16 = jnp.float32, jnp.bfloat16
CONTRACT_LAST = (((1,), (1,)), ((), ()))
CONTRACT_FIRST = (((0,), (0,)), ((), ()))
TOKENS, MODEL, HIDDEN = 4096, 768, 2048
HALF, SHARD = HIDDEN // 2, HIDDEN // 4
TILE = 512
STEPS = TOKENS // TILE
PIECES = 8
ROWS = 3 * MODEL // PIECES
SUB = ROWS // 2
FAR = 4
VMEM_LIMIT = 63 * 2**20


def mm(lhs, rhs, dims=None):
    if dims is None:
        return jnp.dot(lhs, rhs, preferred_element_type=F32)
    return lax.dot_general(lhs, rhs, dims, preferred_element_type=F32)


def tile_backward(x, dy, w1, w3, w2, dw, at=slice(None), first=False, flush=None):
    a = mm(x, w1)
    b = mm(x, w3)
    dh = mm(dy, w2, CONTRACT_LAST)
    s = 0.5 * jnp.tanh(0.5 * a) + 0.5
    sa = a * s
    h = (sa * b).astype(BF16)
    da = (dh * b * (s + sa * (1.0 - s))).astype(BF16)
    db = (dh * sa).astype(BF16)
    if flush is None:
        dx = mm(da, w1, CONTRACT_LAST) + mm(db, w3, CONTRACT_LAST)
    for i, lhs, rhs in ((2, dy, h), (0, x, da), (1, x, db)):
        grad = mm(lhs, rhs, CONTRACT_FIRST)
        dw[i, :, at] = grad if first else dw[i, :, at] + grad
        if flush is not None:
            flush(i)
    if flush is not None:
        dx = mm(da, w1, CONTRACT_LAST) + mm(db, w3, CONTRACT_LAST)
    return dx


def cols(index, width=SHARD):
    return pl.ds(pl.multiple_of(index * width, width), width)


def first_kernel(x_hbm, dy_hbm, s1, s3, s2, g, dx_ref, dxp_out, dw_out, o1, o3, o2, fin_own, fin_other,
                 w1, w3, w2, dw, dxs, gbuf, keep, send_a, recv_a, recv_b, recv_c, xs, dys,
                 own_sem, wd_send, wd_recv, wx_send, wx_recv, wf_send, wf_recv, g_sem, a_send, a_recv, b_send, b_recv,
                 c_send, c_recv, f_send, f_recv, fin_sem, dw_sem, dx_sem, o_sem, x_sem, dy_sem):
    k = pl.program_id(0)
    dp, row, core = lax.axis_index("dp"), lax.axis_index("row"), lax.axis_index("fsdp")
    partner, x_next, y_next = (dp, row, 1 - core), (dp, 1 - row, core), (1 - dp, row, core)
    mine = cols(core)
    theirs = cols(1 - core)
    half = k // STEPS
    slot = k % FAR

    def remote(src, dst, send, recv, device):
        return pltpu.make_async_remote_copy(src_ref=src, dst_ref=dst, send_sem=send, recv_sem=recv, device_id=device, device_id_type=MESH)

    shards = (s1, s3, s2)
    near = (w1.at[0, :, mine], w3.at[0, :, mine], w2.at[0, mine, :])
    far = (w1.at[1, :, mine], w3.at[1, :, mine], w2.at[1, mine, :])
    own = [pltpu.make_async_copy(shards[i], near[i], own_sem.at[i]) for i in range(3)]
    to_partner = [remote(shards[i], near[i], wd_send.at[i], wd_recv.at[i], partner) for i in range(3)]
    to_x = [remote(shards[i], far[i], wx_send.at[i], wx_recv.at[i], x_next) for i in range(3)]
    forward = [remote(far[i], far[i], wf_send.at[i], wf_recv.at[i], partner) for i in range(3)]
    far_out = [pltpu.make_async_copy(w.at[1], o, o_sem.at[i]) for i, (w, o) in enumerate(((w1, o1), (w3, o3), (w2, o2)))]

    def tokens(i):
        rows = pl.ds(pl.multiple_of(jnp.where(i < STEPS, i, i - FAR) * TILE, TILE), TILE)
        return (pltpu.make_async_copy(x_hbm.at[rows, :], xs.at[i % 2], x_sem.at[i % 2]),
                pltpu.make_async_copy(dy_hbm.at[rows, :], dys.at[i % 2], dy_sem.at[i % 2]))

    def load(i):
        return pltpu.make_async_copy(g.at[pl.ds(i * ROWS, ROWS), :], gbuf.at[i % 2], g_sem.at[i % 2])

    def to_a(i):
        return remote(send_a.at[i % 4], recv_a.at[i], a_send.at[i % 4], a_recv.at[i], partner)

    def to_b(i):
        part = keep.at[i, pl.ds(pl.multiple_of((1 - dp) * SUB, SUB), SUB), :]
        return remote(part, recv_b.at[i], b_send.at[i], b_recv.at[i], y_next)

    stay = pl.ds(pl.multiple_of(dp * SUB, SUB), SUB)

    def to_c(i):
        return remote(keep.at[i, stay, cols(1 - row)], recv_c.at[i], c_send.at[i], c_recv.at[i], x_next)

    def to_f(i):
        return remote(keep.at[i, stay, cols(row)], fin_other.at[i], f_send.at[i], f_recv.at[i], y_next)

    def own_fin(i):
        return pltpu.make_async_copy(keep.at[i, stay, cols(row)], fin_own.at[i], fin_sem.at[i])

    def dx_out(i):
        return pltpu.make_async_copy(dxs.at[i], dxp_out.at[i], dx_sem.at[i])

    def cast(i):
        load(i).wait()
        for part in range(2):
            here = pl.ds(part * SHARD, SHARD)
            keep[i, :, here] = gbuf[i % 2, :, pl.ds(pl.multiple_of(part * HALF + core * SHARD, SHARD), SHARD)].astype(BF16)
            send_a[i % 4, :, here] = gbuf[i % 2, :, pl.ds(pl.multiple_of(part * HALF + (1 - core) * SHARD, SHARD), SHARD)].astype(BF16)
        to_a(i).start()

    def chip_sum(i):
        to_a(i).wait_recv()
        keep[i] = keep[i] + recv_a[i]
        to_b(i).start()

    def pair_sum(i):
        to_b(i).wait_recv()
        keep[i, stay, :] = keep[i, stay, :] + recv_b[i]
        to_c(i).start()

    def whole_sum(i):
        to_c(i).wait_recv()
        keep[i, stay, cols(row)] = keep[i, stay, cols(row)] + recv_c[i]
        to_f(i).start()
        own_fin(i).start()

    @pl.when(k == 0)
    def _():
        barrier = pltpu.get_barrier_semaphore()
        for device in (partner, x_next, y_next):
            pl.semaphore_signal(barrier, inc=1, device_id=device, device_id_type=MESH)
        for copy in tokens(0):
            copy.start()
        for copy in own:
            copy.start()
        pl.semaphore_wait(barrier, 3)
        for copy in to_x:
            copy.start()
        for copy in tokens(0):
            copy.wait()
        for copy in own:
            copy.wait()
        for copy in to_partner:
            copy.start()
        load(0).start()
        load(1).start()
        for copy in tokens(1):
            copy.start()
        dxs[0] = tile_backward(xs[0], dys[0], w1[0, :, mine], w3[0, :, mine], w2[0, mine, :], dw, mine, first=True)
        cast(0)
        load(2).start()
        cast(1)
        load(3).start()
        for copy in to_partner:
            copy.wait_recv()
        dxs[0] += tile_backward(xs[0], dys[0], w1[0, :, theirs], w3[0, :, theirs], w2[0, theirs, :], dw, theirs, first=True)

    @pl.when(k > 0)
    def _():
        for copy in tokens(k):
            copy.wait()

        @pl.when(k < STEPS + FAR - 1)
        def _():
            for copy in tokens(k + 1):
                copy.start()

    @pl.when(k == 1)
    def _():
        chip_sum(0)

    @pl.when(jnp.logical_and(k > 0, k < PIECES))
    def _():
        chip_sum(k)

        @pl.when(k <= PIECES - 2)
        def _():
            @pl.when(k >= 3)
            def _():
                to_a(k - 3).wait_send()
            cast(k + 1)

            @pl.when(k <= PIECES - 4)
            def _():
                load(k + 3).start()

        @pl.when(k <= FAR)
        def _():
            dx_out(k - 1).start()

        @pl.when(k >= FAR)
        def _():
            dx_out(k - FAR).wait()

        for at, i in ((3, 0), (6, 1)):
            @pl.when(k == at)
            def _():
                to_x[i].wait_recv()
                forward[i].start()

    @pl.when(jnp.logical_and(k >= 3, k <= PIECES + 1))
    def _():
        @pl.when(k == 3)
        def _():
            pair_sum(0)
        pair_sum(k - 2)

    @pl.when(k >= STEPS)
    def _():
        for at, pieces in enumerate(((0, 1), (2, 3), (4, 5, 6), (7,))):
            @pl.when(k == STEPS + at)
            def _():
                for i in pieces:
                    whole_sum(i)

        @pl.when(k == STEPS)
        def _():
            for i in range(3):
                pltpu.make_async_copy(dw.at[i], dw_out.at[0, i], dw_sem.at[i]).wait()
            dw[...] = jnp.zeros_like(dw)
            for i in range(3):
                forward[i].wait_recv()
                far_out[i].start()

    def finish(flush):
        dx = tile_backward(xs[k % 2], dys[k % 2], w1[half], w3[half], w2[half], dw, flush=flush)
        total = dx + jnp.where(k >= STEPS, dxs[slot], 0.0)
        dxs[slot] = total
        dx_ref[...] = total.astype(BF16)

    ends = jnp.logical_or(k == STEPS - 1, k == STEPS + FAR - 1)

    @pl.when(jnp.logical_and(k > 0, jnp.logical_not(ends)))
    def _():
        finish(None)

    @pl.when(ends)
    def _():
        finish(lambda i: pltpu.make_async_copy(dw.at[i], dw_out.at[half, i], dw_sem.at[i]).start())

    @pl.when(k == STEPS - 1)
    def _():
        to_x[2].wait_recv()
        forward[2].start()

    @pl.when(k == STEPS + FAR - 1)
    def _():
        for i in range(3):
            to_partner[i].wait_send()
            to_x[i].wait_send()
            forward[i].wait_send()
            far_out[i].wait()
        for i in range(PIECES - 4, PIECES):
            to_a(i).wait_send()
        for i in range(PIECES):
            to_b(i).wait_send()
            to_c(i).wait_send()
            own_fin(i).wait()
            to_f(i).wait()
        for i in range(3):
            pltpu.make_async_copy(dw.at[i], dw_out.at[1, i], dw_sem.at[i]).wait()


def second_kernel(x_hbm, dy_hbm, o1, o3, o2, dxp, dxq, fin_own, fin_other, dw_part, dx_ref, next_ref, dw_out,
                  w1, w3, w2, dw, near_buf, far_buf, xs, dys, dx_near, dx_done, own, other,
                  in_sem, w_sem, near_in_sem, near_out_sem, far_in_sem, far_out_sem):
    k = pl.program_id(0)
    dp, row = lax.axis_index("dp"), lax.axis_index("row")
    slot = k % 2
    near_in = [pltpu.make_async_copy(dw_part.at[0, i], near_buf.at[i], near_in_sem.at[i]) for i in range(3)]
    near_out = [pltpu.make_async_copy(near_buf.at[i], dw_out.at[i, :, cols(row, HALF)], near_out_sem.at[i]) for i in range(3)]
    far_in = [pltpu.make_async_copy(dw_part.at[1, i], far_buf.at[i], far_in_sem.at[i]) for i in range(3)]
    far_out = [pltpu.make_async_copy(dw.at[i], dw_out.at[i, :, cols(1 - row, HALF)], far_out_sem.at[i]) for i in range(3)]
    weights = [pltpu.make_async_copy(o, w, w_sem.at[i]) for i, (o, w) in enumerate(((o1, w1), (o3, w3), (o2, w2)))]
    group = PIECES // (STEPS - FAR)

    def inputs(t):
        rows = pl.ds(pl.multiple_of(t * TILE, TILE), TILE)
        pieces = pl.ds(t * group, group)
        pairs = ((x_hbm.at[rows, :], xs), (dy_hbm.at[rows, :], dys), (dxp.at[t], dx_near), (dxq.at[rows, :], dx_done),
                 (fin_own.at[pieces], own), (fin_other.at[pieces], other))
        return [pltpu.make_async_copy(src, dst.at[t % 2], in_sem.at[t % 2, i]) for i, (src, dst) in enumerate(pairs)]

    @pl.when(k == 0)
    def _():
        now = inputs(0)
        for copy in now[:2] + weights + now[2:]:
            copy.start()
        dw[...] = jnp.zeros_like(dw)
        for copy in weights:
            copy.wait()

    @pl.when(jnp.logical_and(k > 0, k < STEPS - FAR - 1))
    def _():
        for copy in inputs(k + 1):
            copy.start()

    for copy in inputs(k):
        copy.wait()

    @pl.when(k == 0)
    def _():
        for copy in inputs(1) + far_in + near_in:
            copy.start()

    for i in range(3):
        @pl.when(k == i + 1)
        def _():
            far_in[i].wait()
            dw[i] += far_buf[i]
            near_in[i].wait()
            near_out[i].start()

    def finish(flush):
        dx = tile_backward(xs[slot], dys[slot], w1[...], w3[...], w2[...], dw, flush=flush)
        dx_ref[0] = (dx_near[slot] + dx).astype(BF16)
        dx_ref[1] = dx_done[slot]
        next_ref[:, pl.ds(pl.multiple_of(dp * SUB, SUB), SUB), :] = own[slot].astype(F32)
        next_ref[:, pl.ds(pl.multiple_of((1 - dp) * SUB, SUB), SUB), :] = other[slot].astype(F32)

    @pl.when(k < STEPS - FAR - 1)
    def _():
        finish(None)

    @pl.when(k == STEPS - FAR - 1)
    def _():
        finish(lambda i: far_out[i].start())
        for copy in near_out + far_out:
            copy.wait()


def solution(mesh):
    any_spec = pl.BlockSpec(memory_space=pl.ANY)
    shape = jax.ShapeDtypeStruct
    dma = pltpu.SemaphoreType.DMA
    rest = STEPS - FAR
    tile_flops = 8 * 2 * TILE * MODEL * HALF

    def per_device(x_blk, dy_blk, gate, up, down, g_part):
        g2 = g_part.reshape(3 * MODEL, HIDDEN)
        dxq, dxp, dw_part, o1, o3, o2, fin_own, fin_other = pl.pallas_call(
            first_kernel,
            grid=(STEPS + FAR,),
            in_specs=[any_spec] * 6,
            out_specs=[pl.BlockSpec((TILE, MODEL), lambda t: (jnp.maximum(t - STEPS, 0), 0))] + [any_spec] * 7,
            out_shape=[shape((FAR * TILE, MODEL), BF16), shape((rest, TILE, MODEL), F32), shape((2, 3, MODEL, HALF), F32),
                       shape((MODEL, HALF), BF16), shape((MODEL, HALF), BF16), shape((HALF, MODEL), BF16),
                       shape((PIECES, SUB, SHARD), BF16), shape((PIECES, SUB, SHARD), BF16)],
            scratch_shapes=[
                pltpu.VMEM((2, MODEL, HALF), BF16), pltpu.VMEM((2, MODEL, HALF), BF16), pltpu.VMEM((2, HALF, MODEL), BF16),
                pltpu.VMEM((3, MODEL, HALF), F32), pltpu.VMEM((FAR, TILE, MODEL), F32), pltpu.VMEM((2, ROWS, HIDDEN), F32),
                pltpu.VMEM((PIECES, ROWS, HALF), BF16), pltpu.VMEM((4, ROWS, HALF), BF16), pltpu.VMEM((PIECES, ROWS, HALF), BF16),
                pltpu.VMEM((PIECES, SUB, HALF), BF16), pltpu.VMEM((PIECES, SUB, SHARD), BF16),
                pltpu.VMEM((2, TILE, MODEL), BF16), pltpu.VMEM((2, TILE, MODEL), BF16),
            ] + [dma((3,))] * 7 + [dma((2,)), dma((4,))] + [dma((PIECES,))] * 8 + [dma((3,)), dma((rest,)), dma((3,)), dma((2,)), dma((2,))],
            compiler_params=pltpu.CompilerParams(vmem_limit_bytes=VMEM_LIMIT, collective_id=0, has_side_effects=True),
            cost_estimate=pl.CostEstimate(flops=(STEPS + FAR) * tile_flops, bytes_accessed=100 * 2**20, transcendentals=TOKENS * HALF),
            name="near_and_far",
        )(x_blk, dy_blk, gate, up, down, g2)

        dx, dw_next, dw_local = pl.pallas_call(
            second_kernel,
            grid=(rest,),
            in_specs=[any_spec] * 10,
            out_specs=[pl.BlockSpec((2, TILE, MODEL), lambda t: (0, t, 0)), pl.BlockSpec((PIECES // rest, ROWS, SHARD), lambda t: (t, 0, 0)), any_spec],
            out_shape=[shape((2, TOKENS // 2, MODEL), BF16), shape((PIECES, ROWS, SHARD), F32), shape((3, MODEL, HIDDEN), F32)],
            scratch_shapes=[pltpu.VMEM((MODEL, HALF), BF16), pltpu.VMEM((MODEL, HALF), BF16), pltpu.VMEM((HALF, MODEL), BF16)]
            + [pltpu.VMEM((3, MODEL, HALF), F32)] * 3
            + [pltpu.VMEM((2, TILE, MODEL), BF16), pltpu.VMEM((2, TILE, MODEL), BF16), pltpu.VMEM((2, TILE, MODEL), F32), pltpu.VMEM((2, TILE, MODEL), BF16)]
            + [pltpu.VMEM((2, PIECES // rest, SUB, SHARD), BF16)] * 2 + [dma((2, 6))] + [dma((3,))] * 5,
            compiler_params=pltpu.CompilerParams(vmem_limit_bytes=VMEM_LIMIT),
            cost_estimate=pl.CostEstimate(flops=rest * tile_flops, bytes_accessed=70 * 2**20, transcendentals=TOKENS * HALF // 2),
            name="far_rest",
        )(x_blk, dy_blk, o1, o3, o2, dxp, dxq, fin_own, fin_other, dw_part)
        return dx.reshape(TOKENS, MODEL), dw_next.reshape(3, MODEL, SHARD), dw_local[None]

    return jax.shard_map(
        per_device,
        mesh=mesh,
        in_specs=(P(ALL_AXES, None), P(ALL_AXES, None), P(None, GROUP_AXES), P(None, GROUP_AXES), P(GROUP_AXES, None), P(ALL_AXES, None, None, None)),
        out_specs=(P(ALL_AXES, None), P(None, None, GROUP_AXES), P(ALL_AXES, None, None, None)),
        check_vma=False,
    )
```
